256 devices in a mesh: expert: 64 (over z, x, core), pair: 4 (over y).
Axes of the slice: x: 4, y: 4, z: 8, core: 2. Of those that a mesh axis runs over, the one named last changes fastest.
Arguments:
- tokens: bfloat16 [98304, 2048], P(('expert', 'pair')), may hold values from -6 to 6
- token_ids: int32 [98304], P(('expert', 'pair')), may hold values from 0 to 8191
- table: int32 [8192], replicated, may hold values from 0 to 127
- w_in: bfloat16 [128, 2048, 2048], P('expert', None, 'pair'), may hold values from -0.125 to 0.125
- w_out: bfloat16 [128, 2048, 2048], P('expert', 'pair'), may hold values from -0.125 to 0.125
Outputs:
- mixed: bfloat16 [98304, 2048], P(('expert', 'pair'))
The draws below stay inside these ranges and needn't reach their ends.
All inputs are finite; a program needn't handle non-finite values.
Results may differ from the reference program's by a relative error of at most 0.0085.
Values may be sent and summed in bfloat16 or wider, within the bound.
No kernel may reach another device: no remote copies, remote signals or barrier semaphores. Data moves between devices by JAX's collectives and lax.ppermute only.
A program may use at most 192 MiB of HBM per device.

```python
import math
import jax
import jax.numpy as jnp
import numpy as np
from jax import lax

D = 2048
H = 2048
VOCAB = 8192
TOK_DEV = 384
EXPERTS = 128
CAP = 6
TOKENS = 98304
N_EXPERT = 64
N_PAIR = 4


def touch_ends(result, stream_key, smallest, high):
    index_at = [jax.random.randint(jax.random.fold_in(stream_key, axis), (), 0, length) for axis, length in enumerate(result.shape)]
    longest = result.shape.index(max(result.shape))
    beside = index_at[:longest] + [(index_at[longest] + 1) % result.shape[longest]] + index_at[longest + 1:]
    return result.at[tuple(index_at)].set(smallest).at[tuple(beside)].set(high)


def level_of(key, dims, pieces, low, largest):
    def one(dim, shards_of):
        draws = jax.random.uniform(jax.random.fold_in(jax.random.fold_in(key, 6), dim), (shards_of,), jnp.float32, low / len(pieces), largest / len(pieces))
        return jnp.repeat(jnp.exp(draws), dims[dim] // shards_of).reshape((-1,) + (1,) * (len(dims) - dim - 1))

    gain = one(*pieces[0])
    for cut in pieces[1:]:
        gain = gain * one(*cut)
    return gain


def cumulative_ranks(number_of, lean):
    portions = [(1 << 20) // math.isqrt(grade ** lean) + 1 for grade in range(1, number_of + 1)]
    width = 1 + sum(portions) // (1 << 30)
    return np.cumsum(np.array([max(1, weight // width) for weight in portions]))


def ranked(rng, extent, amount, slope):
    table = cumulative_ranks(amount, slope)
    ticket = jax.random.randint(jax.random.fold_in(rng, 1), extent, 0, int(table[amount - 1]))
    grade = jnp.searchsorted(jnp.asarray(table, jnp.int32), ticket, side="right")
    return jax.random.permutation(jax.random.fold_in(rng, 2), amount)[grade].astype(jnp.int32)


def scatter_about(key, shape, width, reach, pieces=(), kind=jnp.bfloat16):
    array = jax.random.normal(key, shape, jnp.float32) * width
    if len(pieces) > 0:
        array = level_of(key, shape, pieces, -0.22, 0.18) * array
    return jnp.clip(array, min=-reach, max=reach).astype(kind)


def setup_inputs(seed: int = 0) -> dict:
    arg_keys = jax.random.split(jax.random.key(seed), 6)
    tokens = scatter_about(arg_keys[0], (TOKENS, D), 1.0, 6.0, ((0, 256),))
    token_ids = touch_ends(ranked(arg_keys[1], (TOKENS,), VOCAB, 2), jax.random.fold_in(arg_keys[1], 3), 0, VOCAB - 1).astype(jnp.int32)
    table = touch_ends(jax.random.randint(arg_keys[2], (VOCAB,), 0, EXPERTS), jax.random.fold_in(arg_keys[2], 1), 0, EXPERTS - 1).astype(jnp.int32)
    w_in = scatter_about(arg_keys[3], (EXPERTS, D, H), D ** -0.5, 0.125, ((0, 64), (2, 4)))
    w_out = scatter_about(arg_keys[4], (EXPERTS, H, D), H ** -0.5, 0.125, ((0, 64), (1, 4)))
    return {"tokens": tokens, "token_ids": token_ids, "table": table, "w_in": w_in, "w_out": w_out}


def reference(tokens, token_ids, table, w_in, w_out):
    blocks = N_EXPERT * N_PAIR
    quarter = H // N_PAIR
    chosen = jnp.take(table, token_ids, axis=0).astype(jnp.int32).reshape(blocks, TOK_DEV)
    hot = (chosen[:, :, None] == jnp.arange(EXPERTS, dtype=jnp.int32)[None, None, :]).astype(jnp.int32)
    earlier = jnp.cumsum(hot, axis=1) - hot
    rank = jnp.sum(earlier * hot, axis=2)
    kept = rank < CAP
    block_index = jnp.arange(blocks, dtype=jnp.int32)[:, None]
    total_slots = EXPERTS * blocks * CAP
    position = (chosen * blocks + block_index) * CAP + rank
    position = jnp.where(kept, position, total_slots).reshape(-1).astype(jnp.int32)
    buffer = jnp.zeros((total_slots, D), jnp.bfloat16).at[position].set(tokens, mode="drop")
    buffer = buffer.reshape(EXPERTS, blocks * CAP, D)

    def one_expert(items):
        rows, first, second = items
        hidden = jax.nn.relu(jnp.dot(rows, first, preferred_element_type=jnp.float32)).astype(jnp.bfloat16)
        total = jnp.zeros((rows.shape[0], D), jnp.float32)
        for index in range(N_PAIR):
            part = jnp.dot(hidden[:, index * quarter:(index + 1) * quarter],
                           second[index * quarter:(index + 1) * quarter],
                           preferred_element_type=jnp.float32).astype(jnp.bfloat16)
            total = total + lax.optimization_barrier(part).astype(jnp.float32)
        return total.astype(jnp.bfloat16)

    outputs = lax.map(one_expert, (buffer, w_in, w_out)).reshape(total_slots, D)
    safe = jnp.minimum(position, total_slots - 1).astype(jnp.int32)
    picked = jnp.take(outputs, safe, axis=0)
    mixed = jnp.where(kept.reshape(-1)[:, None], picked, jnp.zeros_like(picked))
    return mixed.astype(jnp.bfloat16)
```

```python
import jax
import jax.numpy as jnp
from jax import lax
from jax.sharding import Mesh, PartitionSpec as P

BF = jnp.bfloat16
F32 = jnp.float32


def weight_route():
    rounds = []
    for p in range(4):
        pairs = []
        for c in range(2):
            for y in range(4):
                bits = y ^ p
                h, k = bits >> 1, bits & 1
                pairs.append((c * 4 + y, h * 4 + 2 * c + k))
        rounds.append(pairs)
    return rounds


def on_device(tokens, token_ids, table, w_in, w_out):
    experts = lax.axis_size("g") * lax.axis_size("y")
    tok_rows, width = tokens.shape
    slots = 2 * tok_rows // experts
    quarter = w_out.shape[1]
    half = quarter // 2
    y = lax.axis_index("y")
    own_in, own_out = [], []
    blocks = []
    for p in range(4):
        bits = y ^ p
        h, k = bits >> 1, bits & 1
        blocks.append((
            lax.dynamic_slice(w_in, (k, 0, h * half), (1, width, half))[0],
            lax.dynamic_slice(w_out, (k, h * half, 0), (1, half, width))[0],
        ))
    route = weight_route()
    for p in range(4):
        own_in.append(lax.ppermute(blocks[p][0], ("c", "y"), route[p]))
    for p in range(4):
        own_out.append(lax.ppermute(blocks[p][1], ("c", "y"), route[p]))
    swap = [(0, 1), (1, 0)]
    other_in = [lax.ppermute(b, "c", swap) for b in own_in]
    other_out = [lax.ppermute(b, "c", swap) for b in own_out]
    full_in = jnp.concatenate(own_in + other_in, axis=1)
    full_out = jnp.concatenate(own_out + other_out, axis=0)

    chosen = jnp.take(table, token_ids, axis=0)
    expert_hot = (chosen[:, None] == jnp.arange(experts, dtype=jnp.int32)[None, :]).astype(jnp.int32)
    earlier = jnp.cumsum(expert_hot, axis=0) - expert_hot
    rank_tok = jnp.sum(earlier * expert_hot, axis=1)
    kept = rank_tok < slots
    column = chosen * slots + rank_tok
    placer = (
        (column[:, None] == jnp.arange(experts * slots, dtype=jnp.int32)[None, :]) & kept[:, None]
    ).astype(BF)
    packed = jnp.einsum("ts,td->sd", placer, tokens, preferred_element_type=F32).astype(BF)
    packed = packed.reshape(experts * slots // 2, 2, width)
    arrived = lax.all_to_all(packed, ("g", "y"), split_axis=0, concat_axis=0, tiled=True)
    arrived = arrived.reshape(experts * slots, width)
    hidden = jax.nn.relu(jnp.dot(arrived, full_in, preferred_element_type=F32)).astype(BF)
    result = jnp.dot(hidden, full_out, preferred_element_type=F32).astype(BF)
    result = result.reshape(experts * slots // 2, 2, width)
    returned = lax.all_to_all(result, ("g", "y"), split_axis=0, concat_axis=0, tiled=True)
    flat = returned.reshape(experts * slots, width)
    return jnp.dot(placer, flat, preferred_element_type=F32).astype(BF)


def solution(mesh):
    groups, pair = mesh.shape["expert"], mesh.shape["pair"]
    fine = Mesh(mesh.devices.reshape(groups // 2, 2, pair), ("g", "c", "y"))
    rows = ("g", "c", "y")
    in_specs = (
        P(rows, None),
        P(rows),
        P(),
        P(("g", "c"), None, "y"),
        P(("g", "c"), "y", None),
    )
    return jax.shard_map(
        on_device, mesh=fine, in_specs=in_specs, out_specs=P(rows, None), check_vma=False
    )
```

```python
import jax
import jax.numpy as jnp
from jax import lax
from jax.sharding import Mesh, PartitionSpec as P

BF = jnp.bfloat16
F32 = jnp.float32
SPLIT = 1


def weight_route():
    rounds = []
    for p in range(4):
        pairs = []
        for c in range(2):
            for y in range(4):
                bits = y ^ p
                h, k = bits >> 1, bits & 1
                pairs.append((c * 4 + y, h * 4 + 2 * c + k))
        rounds.append(pairs)
    return rounds


def on_device(tokens, token_ids, table, w_in, w_out):
    experts = lax.axis_size("g") * lax.axis_size("y")
    tok_rows, width = tokens.shape
    slots = 2 * tok_rows // experts
    quarter = w_out.shape[1]
    half = quarter // 2
    y = lax.axis_index("y")
    route = weight_route()
    swap = [(0, 1), (1, 0)]
    cols = width // SPLIT
    own_in, own_out = [], [[] for _ in range(SPLIT)]
    for p in range(4):
        bits = y ^ p
        h, k = bits >> 1, bits & 1
        block = lax.dynamic_slice(w_in, (k, 0, h * half), (1, width, half))[0]
        own_in.append(lax.ppermute(block, ("c", "y"), route[p]))
    for j in range(SPLIT):
        for p in range(4):
            bits = y ^ p
            h, k = bits >> 1, bits & 1
            block = lax.dynamic_slice(w_out, (k, h * half, j * cols), (1, half, cols))[0]
            own_out[j].append(lax.ppermute(block, ("c", "y"), route[p]))
    own_in = jnp.concatenate(own_in, axis=1)
    own_out = [jnp.concatenate(o, axis=0) for o in own_out]
    other_in = lax.ppermute(own_in, "c", swap)
    other_out = []
    for j in range(SPLIT):
        other_out.append(lax.ppermute(own_out[j], "c", swap))

    chosen = jnp.take(table, token_ids, axis=0)
    expert_hot = (chosen[:, None] == jnp.arange(experts, dtype=jnp.int32)[None, :]).astype(jnp.int32)
    earlier = jnp.cumsum(expert_hot, axis=0) - expert_hot
    rank_tok = jnp.sum(earlier * expert_hot, axis=1)
    kept = rank_tok < slots
    column = chosen * slots + rank_tok
    placer = (
        (column[:, None] == jnp.arange(experts * slots, dtype=jnp.int32)[None, :]) & kept[:, None]
    ).astype(BF)
    packed = jnp.einsum("ts,td->sd", placer, tokens, preferred_element_type=F32).astype(BF)
    packed = packed.reshape(experts * slots // 2, 2, width)
    arrived = lax.all_to_all(packed, ("g", "y"), split_axis=0, concat_axis=0, tiled=True)
    arrived = arrived.reshape(experts * slots, width)
    def up(w):
        return jax.nn.relu(jnp.dot(arrived, w, preferred_element_type=F32)).astype(BF)

    hidden_own = up(own_in)
    hidden_other = up(other_in)
    hidden_own, hidden_other = lax.optimization_barrier((hidden_own, hidden_other))
    outs = []
    for j in range(SPLIT):
        result = (
            jnp.dot(hidden_own, own_out[j], preferred_element_type=F32)
            + jnp.dot(hidden_other, other_out[j], preferred_element_type=F32)
        ).astype(BF)
        result = result.reshape(experts * slots // 2, 2, cols)
        returned = lax.all_to_all(result, ("g", "y"), split_axis=0, concat_axis=0, tiled=True)
        flat = returned.reshape(experts * slots, cols)
        outs.append(jnp.dot(placer, flat, preferred_element_type=F32).astype(BF))
    return jnp.concatenate(outs, axis=1)


def solution(mesh):
    groups, pair = mesh.shape["expert"], mesh.shape["pair"]
    fine = Mesh(mesh.devices.reshape(groups // 2, 2, pair), ("g", "c", "y"))
    rows = ("g", "c", "y")
    in_specs = (
        P(rows, None),
        P(rows),
        P(),
        P(("g", "c"), None, "y"),
        P(("g", "c"), "y", None),
    )
    return jax.shard_map(
        on_device, mesh=fine, in_specs=in_specs, out_specs=P(rows, None), check_vma=False
    )
```

```python
import functools

import jax
import jax.numpy as jnp
from jax import lax
from jax.experimental import pallas as pl
from jax.experimental.pallas import tpu as pltpu
from jax.sharding import Mesh, PartitionSpec as P

BF = jnp.bfloat16
F32 = jnp.float32
CUTS = (0, 1536, 2048)


def weight_route():
    rounds = []
    for p in range(4):
        pairs = []
        for c in range(2):
            for y in range(4):
                bits = y ^ p
                h, k = bits >> 1, bits & 1
                pairs.append((c * 4 + y, h * 4 + 2 * c + k))
        rounds.append(pairs)
    return rounds


def pack_kernel(slots, ids_ref, table_ref, tok_ref, packed_ref, place_ref):
    rows, lanes = table_ref.shape
    tok = ids_ref.shape[1]
    pairs = packed_ref.shape[0]
    experts = 2 * pairs // slots
    ids = ids_ref[...]
    low = lax.rem(ids, lanes)
    high = lax.div(ids, lanes)
    low_hot = (lax.broadcasted_iota(jnp.int32, (lanes, tok), 0) == low).astype(F32).astype(BF)
    picked = jnp.dot(table_ref[...].astype(F32).astype(BF), low_hot, preferred_element_type=F32)
    high_hot = lax.broadcasted_iota(jnp.int32, (rows, tok), 0) == high
    chosen = jnp.sum(jnp.where(high_hot, picked, 0.0), axis=0, keepdims=True)
    hot = lax.broadcasted_iota(jnp.int32, (experts, tok), 0).astype(F32) == chosen
    before = (
        lax.broadcasted_iota(jnp.int32, (tok, tok), 0) < lax.broadcasted_iota(jnp.int32, (tok, tok), 1)
    ).astype(F32).astype(BF)
    earlier = jnp.dot(hot.astype(F32).astype(BF), before, preferred_element_type=F32)
    rank = jnp.sum(jnp.where(hot, earlier, 0.0), axis=0, keepdims=True)
    place = jnp.where(rank < slots, chosen * slots + rank, -1.0).astype(jnp.int32)
    place_ref[...] = place
    block = 128

    def step(i, _):
        at = lax.broadcasted_iota(jnp.int32, (block, tok), 0) + i * block
        onehot = (at == place).astype(F32).astype(BF)
        out = jnp.dot(onehot, tok_ref[...], preferred_element_type=F32).astype(BF)
        packed_ref[pl.ds(pl.multiple_of(i * (block // 2), block // 2), block // 2)] = out.reshape(block // 2, 2, out.shape[1])
        return 0

    lax.fori_loop(0, 2 * pairs // block, step, 0)


def pack(token_ids, table, tokens, experts, slots):
    tok, width = tokens.shape
    return pl.pallas_call(
        functools.partial(pack_kernel, slots),
        out_shape=(
            jax.ShapeDtypeStruct((experts * slots // 2, 2, width), BF),
            jax.ShapeDtypeStruct((1, tok), jnp.int32),
        ),
        cost_estimate=pl.CostEstimate(flops=2 * experts * slots * tok * width, bytes_accessed=6 * 1024 * 1024, transcendentals=0),
        compiler_params=pltpu.CompilerParams(vmem_limit_bytes=12 * 1024 * 1024),
        name="pack",
    )(token_ids.reshape(1, tok), table.reshape(-1, 128), tokens)


def flatten_rows(src_ref, dst_ref):
    pairs, _, width = src_ref.shape
    block = 16

    def step(i, _):
        part = src_ref[pl.ds(pl.multiple_of(i * block, block), block)]
        dst_ref[pl.ds(pl.multiple_of(i * 2 * block, 2 * block), 2 * block), :] = part.reshape(2 * block, width)
        return 0

    lax.fori_loop(0, pairs // block, step, 0)


def up_kernel(x_ref, own_ref, other_ref, hidden_ref, rows_ref):
    j = pl.program_id(0)

    @pl.when(j == 0)
    def _():
        flatten_rows(x_ref, rows_ref)

    def run(w_ref):
        out = jnp.dot(rows_ref[...], w_ref[...], preferred_element_type=F32)
        hidden_ref[...] = jnp.maximum(out, 0.0).astype(BF)

    half = pl.num_programs(0) // 2

    @pl.when(j < half)
    def _():
        run(own_ref)

    @pl.when(j >= half)
    def _():
        run(other_ref)


def up(arrived, own, other):
    pairs, _, width = arrived.shape
    units = own.shape[1]
    block = 256
    half = units // block
    return pl.pallas_call(
        up_kernel,
        grid=(2 * half,),
        in_specs=[
            pl.BlockSpec(memory_space=pltpu.VMEM),
            pl.BlockSpec((width, block), lambda j: (0, jnp.minimum(j, half - 1))),
            pl.BlockSpec((width, block), lambda j: (0, jnp.maximum(j - half, 0))),
        ],
        out_specs=pl.BlockSpec((2 * pairs, block), lambda j: (0, j)),
        out_shape=jax.ShapeDtypeStruct((2 * pairs, 2 * units), BF),
        scratch_shapes=[pltpu.VMEM((2 * pairs, width), BF)],
        cost_estimate=pl.CostEstimate(flops=8 * pairs * units * width, bytes_accessed=16 * 1024 * 1024, transcendentals=0),
        compiler_params=pltpu.CompilerParams(vmem_limit_bytes=24 * 1024 * 1024),
        name="up",
    )(arrived, own, other)


def down_kernel(n, hidden_ref, *refs):
    pieces, out_ref, w_ref = refs[:n], refs[-2], refs[-1]
    depth = pieces[0].shape[0]
    for p in range(n):
        w_ref[p * depth:(p + 1) * depth, :] = pieces[p][...]
    out = jnp.dot(hidden_ref[...], w_ref[...], preferred_element_type=F32).astype(BF)
    out_ref[...] = out.reshape(out_ref.shape)


def down(hidden, pieces, start, width, base):
    rows, units = hidden.shape
    depth, cols = pieces[0].shape
    n = len(pieces)
    block = 512
    first = start // block
    specs = [pl.BlockSpec(memory_space=pltpu.VMEM)]
    specs += [pl.BlockSpec((depth, block), lambda j: (0, j)) for _ in range(n)]
    args = [hidden, *pieces]
    aliases = {}
    if base is not None:
        aliases = {len(args): 0}
        args.append(base)
        specs.append(pl.BlockSpec(memory_space=pl.ANY))
    return pl.pallas_call(
        functools.partial(down_kernel, n),
        grid=(cols // block,),
        in_specs=specs,
        out_specs=pl.BlockSpec((rows // 2, 2, block), lambda j: (0, 0, j + first)),
        out_shape=jax.ShapeDtypeStruct((rows // 2, 2, width), BF),
        scratch_shapes=[pltpu.VMEM((units, block), BF)],
        input_output_aliases=aliases,
        cost_estimate=pl.CostEstimate(
            flops=2 * rows * units * cols, bytes_accessed=2 * rows * (units + cols) + 2 * units * cols, transcendentals=0
        ),
        compiler_params=pltpu.CompilerParams(vmem_limit_bytes=20 * 1024 * 1024),
        name="down",
    )(*args)


def mix_kernel(place_ref, back_ref, out_ref, rows_ref, hot_ref):
    @pl.when(pl.program_id(0) == 0)
    def _():
        at = lax.broadcasted_iota(jnp.int32, hot_ref.shape, 0)
        hot_ref[...] = (at == place_ref[...]).astype(F32).astype(BF)

    flatten_rows(back_ref, rows_ref)
    out_ref[...] = lax.dot_general(
        hot_ref[...], rows_ref[...], (((0,), (0,)), ((), ())), preferred_element_type=F32
    ).astype(BF)


def mix(place, returned, block=512):
    pairs, _, cols = returned.shape
    tok = place.shape[1]
    return pl.pallas_call(
        mix_kernel,
        grid=(cols // block,),
        in_specs=[
            pl.BlockSpec((1, tok), lambda j: (0, 0)),
            pl.BlockSpec((pairs, 2, block), lambda j: (0, 0, j)),
        ],
        out_specs=pl.BlockSpec((tok, block), lambda j: (0, j)),
        out_shape=jax.ShapeDtypeStruct((tok, cols), BF),
        scratch_shapes=[pltpu.VMEM((2 * pairs, block), BF), pltpu.VMEM((2 * pairs, tok), BF)],
        cost_estimate=pl.CostEstimate(flops=4 * tok * pairs * cols, bytes_accessed=4 * pairs * cols + 2 * tok * cols, transcendentals=0),
        compiler_params=pltpu.CompilerParams(vmem_limit_bytes=16 * 1024 * 1024),
        name="mix",
    )(place, returned)


def on_device(tokens, token_ids, table, w_in, w_out):
    experts = lax.axis_size("g") * lax.axis_size("y")
    tok_rows, width = tokens.shape
    slots = 2 * tok_rows // experts
    half = w_out.shape[1] // 2
    y = lax.axis_index("y")
    route = weight_route()
    swap = [(0, 1), (1, 0)]
    own_in = []
    for p in range(4):
        h, k = (y ^ p) >> 1, (y ^ p) & 1
        block = lax.dynamic_slice(w_in, (k, 0, h * half), (1, width, half))[0]
        own_in.append(lax.ppermute(block, ("c", "y"), route[p]))
    own_in = jnp.concatenate(own_in, axis=1)
    other_in = lax.ppermute(own_in, "c", swap)
    pieces = []
    for low, high in zip(CUTS[:-1], CUTS[1:]):
        own = []
        for p in range(4):
            h, k = (y ^ p) >> 1, (y ^ p) & 1
            block = lax.dynamic_slice(w_out, (k, h * half, low), (1, half, high - low))[0]
            own.append(lax.ppermute(block, ("c", "y"), route[p]))
        pieces.append(own + [lax.ppermute(o, "c", swap) for o in own])

    packed, place = pack(token_ids, table, tokens, experts, slots)
    arrived = lax.all_to_all(packed, ("g", "y"), split_axis=0, concat_axis=0, tiled=True)
    hidden = up(arrived, own_in, other_in)
    result = None
    for j, low in enumerate(CUTS[:-1]):
        result = down(hidden, pieces[j], low, width, result)
    returned = lax.all_to_all(result, ("g", "y"), split_axis=0, concat_axis=0, tiled=True)
    return mix(place, returned)


def solution(mesh):
    groups, pair = mesh.shape["expert"], mesh.shape["pair"]
    fine = Mesh(mesh.devices.reshape(groups // 2, 2, pair), ("g", "c", "y"))
    rows = ("g", "c", "y")
    in_specs = (
        P(rows, None),
        P(rows),
        P(),
        P(("g", "c"), None, "y"),
        P(("g", "c"), "y", None),
    )
    return jax.shard_map(on_device, mesh=fine, in_specs=in_specs, out_specs=P(rows, None), check_vma=False)
```

```python
import functools

import jax
import jax.numpy as jnp
from jax import lax
from jax.experimental import pallas as pl
from jax.experimental.pallas import tpu as pltpu
from jax.sharding import Mesh, PartitionSpec as P

BF = jnp.bfloat16
F32 = jnp.float32
CUTS = (0, 512, 2048)
PACK_VMEM = 59 * 1024 * 1024
UP_VMEM = 57 * 1024 * 1024


def weight_route():
    rounds = []
    for p in range(4):
        pairs = []
        for c in range(2):
            for y in range(4):
                bits = y ^ p
                h, k = bits >> 1, bits & 1
                pairs.append((c * 4 + y, h * 4 + 2 * c + k))
        rounds.append(pairs)
    return rounds


def pack_kernel(slots, ids_ref, table_ref, tok_ref, packed_ref, place_ref):
    i = pl.program_id(0)
    pairs, _, width = packed_ref.shape
    block = 2 * pairs
    tok = ids_ref.shape[1]

    @pl.when(i == 0)
    def _():
        rows, lanes = table_ref.shape
        experts = pl.num_programs(0) * block // slots
        ids = ids_ref[...]
        low = lax.rem(ids, lanes)
        high = lax.div(ids, lanes)
        low_hot = (lax.broadcasted_iota(jnp.int32, (lanes, tok), 0) == low).astype(F32).astype(BF)
        picked = jnp.dot(table_ref[...].astype(F32).astype(BF), low_hot, preferred_element_type=F32)
        high_hot = lax.broadcasted_iota(jnp.int32, (rows, tok), 0) == high
        chosen = jnp.sum(jnp.where(high_hot, picked, 0.0), axis=0, keepdims=True)
        hot = lax.broadcasted_iota(jnp.int32, (experts, tok), 0).astype(F32) == chosen
        before = (
            lax.broadcasted_iota(jnp.int32, (tok, tok), 0) < lax.broadcasted_iota(jnp.int32, (tok, tok), 1)
        ).astype(F32).astype(BF)
        earlier = jnp.dot(hot.astype(F32).astype(BF), before, preferred_element_type=F32)
        rank = jnp.sum(jnp.where(hot, earlier, 0.0), axis=0, keepdims=True)
        place_ref[...] = jnp.where(rank < slots, chosen * slots + rank, -1.0).astype(jnp.int32)

    at = lax.broadcasted_iota(jnp.int32, (block, tok), 0) + i * block
    onehot = (at == place_ref[...]).astype(F32).astype(BF)
    out = jnp.dot(onehot, tok_ref[...], preferred_element_type=F32).astype(BF)
    packed_ref[...] = out.reshape(pairs, 2, width)


def pack(token_ids, table, tokens, experts, slots):
    tok, width = tokens.shape
    block = 64
    pairs = experts * slots // 2
    return pl.pallas_call(
        functools.partial(pack_kernel, slots),
        grid=(pairs // block,),
        in_specs=[pl.BlockSpec(memory_space=pltpu.VMEM)] * 3,
        out_specs=(
            pl.BlockSpec((block, 2, width), lambda i: (i, 0, 0)),
            pl.BlockSpec((1, tok), lambda i: (0, 0)),
        ),
        out_shape=(
            jax.ShapeDtypeStruct((pairs, 2, width), BF),
            jax.ShapeDtypeStruct((1, tok), jnp.int32),
        ),
        cost_estimate=pl.CostEstimate(flops=4 * pairs * tok * width, bytes_accessed=6 * 1024 * 1024, transcendentals=0),
        compiler_params=pltpu.CompilerParams(vmem_limit_bytes=PACK_VMEM),
        name="pack",
    )(token_ids.reshape(1, tok), table.reshape(-1, 128), tokens)


def flatten_rows(src_ref, dst_ref):
    pairs, _, width = src_ref.shape
    block = 16

    def step(i, _):
        part = src_ref[pl.ds(pl.multiple_of(i * block, block), block)]
        dst_ref[pl.ds(pl.multiple_of(i * 2 * block, 2 * block), 2 * block), :] = part.reshape(2 * block, width)
        return 0

    lax.fori_loop(0, pairs // block, step, 0)


def up_kernel(x_ref, own_ref, other_ref, hidden_ref, rows_ref):
    j = pl.program_id(0)

    @pl.when(j == 0)
    def _():
        flatten_rows(x_ref, rows_ref)

    def run(w_ref):
        out = jnp.dot(rows_ref[...], w_ref[...], preferred_element_type=F32)
        hidden_ref[...] = jnp.maximum(out, 0.0).astype(BF)

    half = pl.num_programs(0) // 2

    @pl.when(j < half)
    def _():
        run(own_ref)

    @pl.when(j >= half)
    def _():
        run(other_ref)


def up(arrived, own, other):
    pairs, _, width = arrived.shape
    units = own.shape[1]
    block = 256
    half = units // block
    return pl.pallas_call(
        up_kernel,
        grid=(2 * half,),
        in_specs=[
            pl.BlockSpec(memory_space=pltpu.VMEM),
            pl.BlockSpec((width, block), lambda j: (0, jnp.minimum(j, half - 1))),
            pl.BlockSpec((width, block), lambda j: (0, jnp.maximum(j - half, 0))),
        ],
        out_specs=pl.BlockSpec((2 * pairs, block), lambda j: (0, j)),
        out_shape=jax.ShapeDtypeStruct((2 * pairs, 2 * units), BF),
        scratch_shapes=[pltpu.VMEM((2 * pairs, width), BF)],
        cost_estimate=pl.CostEstimate(flops=8 * pairs * units * width, bytes_accessed=16 * 1024 * 1024, transcendentals=0),
        compiler_params=pltpu.CompilerParams(vmem_limit_bytes=UP_VMEM),
        name="up",
    )(arrived, own, other)


def down_kernel(n, hidden_ref, *refs):
    pieces, out_ref, w_ref = refs[:n], refs[-2], refs[-1]
    depth = pieces[0].shape[0]
    for p in range(n):
        w_ref[p * depth:(p + 1) * depth, :] = pieces[p][...]
    out = jnp.dot(hidden_ref[...], w_ref[...], preferred_element_type=F32).astype(BF)
    out_ref[...] = out.reshape(out_ref.shape)


def down(hidden, pieces):
    rows, units = hidden.shape
    depth, cols = pieces[0].shape
    n = len(pieces)
    block = 512
    return pl.pallas_call(
        functools.partial(down_kernel, n),
        grid=(cols // block,),
        in_specs=[pl.BlockSpec(memory_space=pltpu.VMEM)] + [pl.BlockSpec((depth, block), lambda j: (0, j)) for _ in range(n)],
        out_specs=pl.BlockSpec((rows // 2, 2, block), lambda j: (0, 0, j)),
        out_shape=jax.ShapeDtypeStruct((rows // 2, 2, cols), BF),
        scratch_shapes=[pltpu.VMEM((units, block), BF)],
        cost_estimate=pl.CostEstimate(
            flops=2 * rows * units * cols, bytes_accessed=2 * rows * (units + cols) + 2 * units * cols, transcendentals=0
        ),
        compiler_params=pltpu.CompilerParams(vmem_limit_bytes=20 * 1024 * 1024),
        name="down",
    )(hidden, *pieces)


def hot_kernel(place_ref, hot_ref):
    at = lax.broadcasted_iota(jnp.int32, hot_ref.shape, 0)
    hot_ref[...] = (at == place_ref[...]).astype(F32).astype(BF)


def hots(place, rows):
    tok = place.shape[1]
    return pl.pallas_call(
        hot_kernel,
        out_shape=jax.ShapeDtypeStruct((rows, tok), BF),
        compiler_params=pltpu.CompilerParams(vmem_limit_bytes=8 * 1024 * 1024),
        name="hots",
    )(place)


def mix_kernel(hot_ref, back_ref, *refs):
    out_ref, rows_ref = refs[-2:]
    flatten_rows(back_ref, rows_ref)
    out_ref[...] = lax.dot_general(
        hot_ref[...], rows_ref[...], (((0,), (0,)), ((), ())), preferred_element_type=F32
    ).astype(BF)


def mix(hot, returned, start, width, base):
    pairs, _, cols = returned.shape
    tok = hot.shape[1]
    block = 512
    first = start // block
    specs = [
        pl.BlockSpec(memory_space=pltpu.VMEM),
        pl.BlockSpec((pairs, 2, block), lambda j: (0, 0, j)),
    ]
    args, aliases = [hot, returned], {}
    if base is not None:
        aliases = {2: 0}
        args.append(base)
        specs.append(pl.BlockSpec(memory_space=pl.ANY))
    return pl.pallas_call(
        mix_kernel,
        grid=(cols // block,),
        in_specs=specs,
        out_specs=pl.BlockSpec((tok, block), lambda j: (0, j + first)),
        out_shape=jax.ShapeDtypeStruct((tok, width), BF),
        scratch_shapes=[pltpu.VMEM((2 * pairs, block), BF)],
        input_output_aliases=aliases,
        cost_estimate=pl.CostEstimate(flops=4 * tok * pairs * cols, bytes_accessed=4 * pairs * cols + 2 * tok * cols, transcendentals=0),
        compiler_params=pltpu.CompilerParams(vmem_limit_bytes=16 * 1024 * 1024),
        name="mix",
    )(*args)


def on_device(tokens, token_ids, table, w_in, w_out):
    experts = lax.axis_size("g") * lax.axis_size("y")
    tok_rows, width = tokens.shape
    slots = 2 * tok_rows // experts
    half = w_out.shape[1] // 2
    y = lax.axis_index("y")
    route = weight_route()
    swap = [(0, 1), (1, 0)]
    own_in = []
    for p in range(4):
        h, k = (y ^ p) >> 1, (y ^ p) & 1
        block = lax.dynamic_slice(w_in, (k, 0, h * half), (1, width, half))[0]
        own_in.append(lax.ppermute(block, ("c", "y"), route[p]))
    other_in = [lax.ppermute(o, "c", swap) for o in own_in]
    own_in = jnp.concatenate(own_in, axis=1)
    other_in = jnp.concatenate(other_in, axis=1)
    pieces = []
    for low, high in zip(CUTS[:-1], CUTS[1:]):
        own = []
        for p in range(4):
            h, k = (y ^ p) >> 1, (y ^ p) & 1
            block = lax.dynamic_slice(w_out, (k, h * half, low), (1, half, high - low))[0]
            own.append(lax.ppermute(block, ("c", "y"), route[p]))
        pieces.append(own + [lax.ppermute(o, "c", swap) for o in own])

    packed, place = pack(token_ids, table, tokens, experts, slots)
    arrived = lax.all_to_all(packed, ("g", "y"), split_axis=0, concat_axis=0, tiled=True)
    hidden = up(arrived, own_in, other_in)
    returned = []
    for j in range(len(CUTS) - 1):
        result = down(hidden, pieces[j])
        returned.append(lax.all_to_all(result, ("g", "y"), split_axis=0, concat_axis=0, tiled=True))
    hot = hots(place, experts * slots)
    mixed = None
    for j, low in enumerate(CUTS[:-1]):
        mixed = mix(hot, returned[j], low, width, mixed)
    return mixed


def solution(mesh):
    groups, pair = mesh.shape["expert"], mesh.shape["pair"]
    fine = Mesh(mesh.devices.reshape(groups // 2, 2, pair), ("g", "c", "y"))
    rows = ("g", "c", "y")
    in_specs = (
        P(rows, None),
        P(rows),
        P(),
        P(("g", "c"), None, "y"),
        P(("g", "c"), "y", None),
    )
    return jax.shard_map(on_device, mesh=fine, in_specs=in_specs, out_specs=P(rows, None), check_vma=False)
```

```python
import functools

import jax
import jax.numpy as jnp
from jax import lax
from jax.experimental import pallas as pl
from jax.experimental.pallas import tpu as pltpu
from jax.sharding import Mesh, PartitionSpec as P

BF = jnp.bfloat16
F32 = jnp.float32
CUTS = (0, 512, 2048)


def weight_route():
    rounds = []
    for p in range(4):
        pairs = []
        for c in range(2):
            for y in range(4):
                bits = y ^ p
                h, k = bits >> 1, bits & 1
                pairs.append((c * 4 + y, h * 4 + 2 * c + k))
        rounds.append(pairs)
    return rounds


def pack_kernel(slots, ids_ref, table_ref, tok_ref, packed_ref, place_ref):
    rows, lanes = table_ref.shape
    tok = ids_ref.shape[1]
    pairs = packed_ref.shape[0]
    experts = 2 * pairs // slots
    ids = ids_ref[...]
    low = lax.rem(ids, lanes)
    high = lax.div(ids, lanes)
    low_hot = (lax.broadcasted_iota(jnp.int32, (lanes, tok), 0) == low).astype(F32).astype(BF)
    picked = jnp.dot(table_ref[...].astype(F32).astype(BF), low_hot, preferred_element_type=F32)
    high_hot = lax.broadcasted_iota(jnp.int32, (rows, tok), 0) == high
    chosen = jnp.sum(jnp.where(high_hot, picked, 0.0), axis=0, keepdims=True)
    hot = lax.broadcasted_iota(jnp.int32, (experts, tok), 0).astype(F32) == chosen
    before = (
        lax.broadcasted_iota(jnp.int32, (tok, tok), 0) < lax.broadcasted_iota(jnp.int32, (tok, tok), 1)
    ).astype(F32).astype(BF)
    earlier = jnp.dot(hot.astype(F32).astype(BF), before, preferred_element_type=F32)
    rank = jnp.sum(jnp.where(hot, earlier, 0.0), axis=0, keepdims=True)
    place = jnp.where(rank < slots, chosen * slots + rank, -1.0).astype(jnp.int32)
    place_ref[...] = place
    block = 128

    def step(i, _):
        at = lax.broadcasted_iota(jnp.int32, (block, tok), 0) + i * block
        onehot = (at == place).astype(F32).astype(BF)
        out = jnp.dot(onehot, tok_ref[...], preferred_element_type=F32).astype(BF)
        packed_ref[pl.ds(pl.multiple_of(i * (block // 2), block // 2), block // 2)] = out.reshape(block // 2, 2, out.shape[1])
        return 0

    lax.fori_loop(0, 2 * pairs // block, step, 0)


def pack(token_ids, table, tokens, experts, slots):
    tok, width = tokens.shape
    return pl.pallas_call(
        functools.partial(pack_kernel, slots),
        out_shape=(
            jax.ShapeDtypeStruct((experts * slots // 2, 2, width), BF),
            jax.ShapeDtypeStruct((1, tok), jnp.int32),
        ),
        cost_estimate=pl.CostEstimate(flops=2 * experts * slots * tok * width, bytes_accessed=6 * 1024 * 1024, transcendentals=0),
        compiler_params=pltpu.CompilerParams(vmem_limit_bytes=12 * 1024 * 1024),
        name="pack",
    )(token_ids.reshape(1, tok), table.reshape(-1, 128), tokens)


def flatten_rows(src_ref, dst_ref):
    pairs, _, width = src_ref.shape
    block = 16

    def step(i, _):
        part = src_ref[pl.ds(pl.multiple_of(i * block, block), block)]
        dst_ref[pl.ds(pl.multiple_of(i * 2 * block, 2 * block), 2 * block), :] = part.reshape(2 * block, width)
        return 0

    lax.fori_loop(0, pairs // block, step, 0)


def up_kernel(n, x_ref, *refs):
    pieces = refs[:n]
    hidden_ref, rows_ref, w_ref, sems = refs[n:]
    copies = [pltpu.make_async_copy(pieces[p], w_ref.at[p], sems.at[p]) for p in range(n)]
    for copy in copies:
        copy.start()
    flatten_rows(x_ref, rows_ref)
    units = w_ref.shape[2]
    for p in range(n):
        copies[p].wait()
        out = jnp.dot(rows_ref[...], w_ref[p], preferred_element_type=F32)
        hidden_ref[:, p * units:(p + 1) * units] = jnp.maximum(out, 0.0).astype(BF)


def up(arrived, pieces):
    pairs, _, width = arrived.shape
    n = len(pieces)
    units = pieces[0].shape[1]
    return pl.pallas_call(
        functools.partial(up_kernel, n),
        in_specs=[pl.BlockSpec(memory_space=pltpu.VMEM)] + [pl.BlockSpec(memory_space=pltpu.HBM)] * n,
        out_specs=pl.BlockSpec(memory_space=pltpu.VMEM),
        out_shape=jax.ShapeDtypeStruct((2 * pairs, n * units), BF),
        scratch_shapes=[
            pltpu.VMEM((2 * pairs, width), BF),
            pltpu.VMEM((n, width, units), BF),
            pltpu.SemaphoreType.DMA((n,)),
        ],
        cost_estimate=pl.CostEstimate(flops=4 * pairs * n * units * width, bytes_accessed=16 * 1024 * 1024, transcendentals=0),
        compiler_params=pltpu.CompilerParams(vmem_limit_bytes=32 * 1024 * 1024),
        name="up",
    )(arrived, *pieces)


def down_kernel(n, hidden_ref, *refs):
    pieces, out_ref, w_ref = refs[:n], refs[-2], refs[-1]
    depth = pieces[0].shape[0]
    for p in range(n):
        w_ref[p * depth:(p + 1) * depth, :] = pieces[p][...]
    out = jnp.dot(hidden_ref[...], w_ref[...], preferred_element_type=F32).astype(BF)
    out_ref[...] = out.reshape(out_ref.shape)


def down(hidden, pieces):
    rows, units = hidden.shape
    depth, cols = pieces[0].shape
    n = len(pieces)
    block = 512
    return pl.pallas_call(
        functools.partial(down_kernel, n),
        grid=(cols // block,),
        in_specs=[pl.BlockSpec(memory_space=pltpu.VMEM)] + [pl.BlockSpec((depth, block), lambda j: (0, j)) for _ in range(n)],
        out_specs=pl.BlockSpec((rows // 2, 2, block), lambda j: (0, 0, j)),
        out_shape=jax.ShapeDtypeStruct((rows // 2, 2, cols), BF),
        scratch_shapes=[pltpu.VMEM((units, block), BF)],
        cost_estimate=pl.CostEstimate(
            flops=2 * rows * units * cols, bytes_accessed=2 * rows * (units + cols) + 2 * units * cols, transcendentals=0
        ),
        compiler_params=pltpu.CompilerParams(vmem_limit_bytes=20 * 1024 * 1024),
        name="down",
    )(hidden, *pieces)


def hot_kernel(place_ref, hot_ref):
    at = lax.broadcasted_iota(jnp.int32, hot_ref.shape, 0)
    hot_ref[...] = (at == place_ref[...]).astype(F32).astype(BF)


def hots(place, rows):
    tok = place.shape[1]
    return pl.pallas_call(
        hot_kernel,
        out_shape=jax.ShapeDtypeStruct((rows, tok), BF),
        compiler_params=pltpu.CompilerParams(vmem_limit_bytes=8 * 1024 * 1024),
        name="hots",
    )(place)


def mix_kernel(hot_ref, back_ref, *refs):
    out_ref, rows_ref = refs[-2:]
    flatten_rows(back_ref, rows_ref)
    out_ref[...] = lax.dot_general(
        hot_ref[...], rows_ref[...], (((0,), (0,)), ((), ())), preferred_element_type=F32
    ).astype(BF)


def mix(hot, returned, start, width, base):
    pairs, _, cols = returned.shape
    tok = hot.shape[1]
    block = 512
    first = start // block
    specs = [
        pl.BlockSpec(memory_space=pltpu.VMEM),
        pl.BlockSpec((pairs, 2, block), lambda j: (0, 0, j)),
    ]
    args, aliases = [hot, returned], {}
    if base is not None:
        aliases = {2: 0}
        args.append(base)
        specs.append(pl.BlockSpec(memory_space=pl.ANY))
    return pl.pallas_call(
        mix_kernel,
        grid=(cols // block,),
        in_specs=specs,
        out_specs=pl.BlockSpec((tok, block), lambda j: (0, j + first)),
        out_shape=jax.ShapeDtypeStruct((tok, width), BF),
        scratch_shapes=[pltpu.VMEM((2 * pairs, block), BF)],
        input_output_aliases=aliases,
        cost_estimate=pl.CostEstimate(flops=4 * tok * pairs * cols, bytes_accessed=4 * pairs * cols + 2 * tok * cols, transcendentals=0),
        compiler_params=pltpu.CompilerParams(vmem_limit_bytes=16 * 1024 * 1024),
        name="mix",
    )(*args)


def on_device(tokens, token_ids, table, w_in, w_out):
    experts = lax.axis_size("g") * lax.axis_size("y")
    tok_rows, width = tokens.shape
    slots = 2 * tok_rows // experts
    half = w_out.shape[1] // 2
    y = lax.axis_index("y")
    route = weight_route()
    swap = [(0, 1), (1, 0)]
    own_in, other_in = [], []
    for p in range(4):
        h, k = (y ^ p) >> 1, (y ^ p) & 1
        block = lax.dynamic_slice(w_in, (k, 0, h * half), (1, width, half))[0]
        own_in.append(lax.ppermute(block, ("c", "y"), route[p]))
        other_in.append(lax.ppermute(own_in[p], "c", swap))
    pieces = []
    for low, high in zip(CUTS[:-1], CUTS[1:]):
        own = []
        for p in range(4):
            h, k = (y ^ p) >> 1, (y ^ p) & 1
            block = lax.dynamic_slice(w_out, (k, h * half, low), (1, half, high - low))[0]
            own.append(lax.ppermute(block, ("c", "y"), route[p]))
        pieces.append(own + [lax.ppermute(o, "c", swap) for o in own])

    packed, place = pack(token_ids, table, tokens, experts, slots)
    arrived = lax.all_to_all(packed, ("g", "y"), split_axis=0, concat_axis=0, tiled=True)
    hidden = up(arrived, own_in + other_in)
    returned = []
    for j in range(len(CUTS) - 1):
        result = down(hidden, pieces[j])
        returned.append(lax.all_to_all(result, ("g", "y"), split_axis=0, concat_axis=0, tiled=True))
    hot = hots(place, experts * slots)
    mixed = None
    for j, low in enumerate(CUTS[:-1]):
        mixed = mix(hot, returned[j], low, width, mixed)
    return mixed


def solution(mesh):
    groups, pair = mesh.shape["expert"], mesh.shape["pair"]
    fine = Mesh(mesh.devices.reshape(groups // 2, 2, pair), ("g", "c", "y"))
    rows = ("g", "c", "y")
    in_specs = (
        P(rows, None),
        P(rows),
        P(),
        P(("g", "c"), None, "y"),
        P(("g", "c"), "y", None),
    )
    return jax.shard_map(on_device, mesh=fine, in_specs=in_specs, out_specs=P(rows, None), check_vma=False)
```

```python
import functools

import jax
import jax.numpy as jnp
from jax import lax
from jax.experimental import pallas as pl
from jax.experimental.pallas import tpu as pltpu
from jax.sharding import Mesh, PartitionSpec as P

BF = jnp.bfloat16
F32 = jnp.float32
CUTS = (0, 512, 2048)
UP_VMEM = 46 * 1024 * 1024


def weight_route():
    rounds = []
    for p in range(4):
        pairs = []
        for c in range(2):
            for y in range(4):
                bits = y ^ p
                h, k = bits >> 1, bits & 1
                pairs.append((c * 4 + y, h * 4 + 2 * c + k))
        rounds.append(pairs)
    return rounds


def pack_kernel(slots, ids_ref, table_ref, tok_ref, packed_ref, place_ref):
    rows, lanes = table_ref.shape
    tok = ids_ref.shape[1]
    pairs = packed_ref.shape[0]
    experts = 2 * pairs // slots
    ids = ids_ref[...]
    low = lax.rem(ids, lanes)
    high = lax.div(ids, lanes)
    low_hot = (lax.broadcasted_iota(jnp.int32, (lanes, tok), 0) == low).astype(F32).astype(BF)
    picked = jnp.dot(table_ref[...].astype(F32).astype(BF), low_hot, preferred_element_type=F32)
    high_hot = lax.broadcasted_iota(jnp.int32, (rows, tok), 0) == high
    chosen = jnp.sum(jnp.where(high_hot, picked, 0.0), axis=0, keepdims=True)
    hot = lax.broadcasted_iota(jnp.int32, (experts, tok), 0).astype(F32) == chosen
    before = (
        lax.broadcasted_iota(jnp.int32, (tok, tok), 0) < lax.broadcasted_iota(jnp.int32, (tok, tok), 1)
    ).astype(F32).astype(BF)
    earlier = jnp.dot(hot.astype(F32).astype(BF), before, preferred_element_type=F32)
    rank = jnp.sum(jnp.where(hot, earlier, 0.0), axis=0, keepdims=True)
    place = jnp.where(rank < slots, chosen * slots + rank, -1.0).astype(jnp.int32)
    place_ref[...] = place
    block = 128

    def step(i, _):
        at = lax.broadcasted_iota(jnp.int32, (block, tok), 0) + i * block
        onehot = (at == place).astype(F32).astype(BF)
        out = jnp.dot(onehot, tok_ref[...], preferred_element_type=F32).astype(BF)
        packed_ref[pl.ds(pl.multiple_of(i * (block // 2), block // 2), block // 2)] = out.reshape(block // 2, 2, out.shape[1])
        return 0

    lax.fori_loop(0, 2 * pairs // block, step, 0)


def pack(token_ids, table, tokens, experts, slots):
    tok, width = tokens.shape
    return pl.pallas_call(
        functools.partial(pack_kernel, slots),
        out_shape=(
            jax.ShapeDtypeStruct((experts * slots // 2, 2, width), BF),
            jax.ShapeDtypeStruct((1, tok), jnp.int32),
        ),
        cost_estimate=pl.CostEstimate(flops=2 * experts * slots * tok * width, bytes_accessed=6 * 1024 * 1024, transcendentals=0),
        compiler_params=pltpu.CompilerParams(vmem_limit_bytes=12 * 1024 * 1024),
        name="pack",
    )(token_ids.reshape(1, tok), table.reshape(-1, 128), tokens)


def flatten_rows(src_ref, dst_ref):
    pairs, _, width = src_ref.shape
    block = 16

    def step(i, _):
        part = src_ref[pl.ds(pl.multiple_of(i * block, block), block)]
        dst_ref[pl.ds(pl.multiple_of(i * 2 * block, 2 * block), 2 * block), :] = part.reshape(2 * block, width)
        return 0

    lax.fori_loop(0, pairs // block, step, 0)


def up_kernel(x_ref, own_ref, other_ref, hidden_ref, rows_ref):
    j = pl.program_id(0)

    @pl.when(j == 0)
    def _():
        flatten_rows(x_ref, rows_ref)

    def run(w_ref):
        out = jnp.dot(rows_ref[...], w_ref[...], preferred_element_type=F32)
        hidden_ref[...] = jnp.maximum(out, 0.0).astype(BF)

    half = pl.num_programs(0) // 2

    @pl.when(j < half)
    def _():
        run(own_ref)

    @pl.when(j >= half)
    def _():
        run(other_ref)


def up(arrived, own, other):
    pairs, _, width = arrived.shape
    units = own.shape[1]
    block = 256
    half = units // block
    return pl.pallas_call(
        up_kernel,
        grid=(2 * half,),
        in_specs=[
            pl.BlockSpec(memory_space=pltpu.VMEM),
            pl.BlockSpec((width, block), lambda j: (0, jnp.minimum(j, half - 1))),
            pl.BlockSpec((width, block), lambda j: (0, jnp.maximum(j - half, 0))),
        ],
        out_specs=pl.BlockSpec((2 * pairs, block), lambda j: (0, j)),
        out_shape=jax.ShapeDtypeStruct((2 * pairs, 2 * units), BF),
        scratch_shapes=[pltpu.VMEM((2 * pairs, width), BF)],
        cost_estimate=pl.CostEstimate(flops=8 * pairs * units * width, bytes_accessed=16 * 1024 * 1024, transcendentals=0),
        compiler_params=pltpu.CompilerParams(vmem_limit_bytes=UP_VMEM),
        name="up",
    )(arrived, own, other)


def down_kernel(n, hidden_ref, *refs):
    pieces, out_ref, w_ref = refs[:n], refs[-2], refs[-1]
    depth = pieces[0].shape[0]
    for p in range(n):
        w_ref[p * depth:(p + 1) * depth, :] = pieces[p][...]
    out = jnp.dot(hidden_ref[...], w_ref[...], preferred_element_type=F32).astype(BF)
    out_ref[...] = out.reshape(out_ref.shape)


def down(hidden, pieces):
    rows, units = hidden.shape
    depth, cols = pieces[0].shape
    n = len(pieces)
    block = 512
    return pl.pallas_call(
        functools.partial(down_kernel, n),
        grid=(cols // block,),
        in_specs=[pl.BlockSpec(memory_space=pltpu.VMEM)] + [pl.BlockSpec((depth, block), lambda j: (0, j)) for _ in range(n)],
        out_specs=pl.BlockSpec((rows // 2, 2, block), lambda j: (0, 0, j)),
        out_shape=jax.ShapeDtypeStruct((rows // 2, 2, cols), BF),
        scratch_shapes=[pltpu.VMEM((units, block), BF)],
        cost_estimate=pl.CostEstimate(
            flops=2 * rows * units * cols, bytes_accessed=2 * rows * (units + cols) + 2 * units * cols, transcendentals=0
        ),
        compiler_params=pltpu.CompilerParams(vmem_limit_bytes=20 * 1024 * 1024),
        name="down",
    )(hidden, *pieces)


def hot_kernel(place_ref, hot_ref):
    at = lax.broadcasted_iota(jnp.int32, hot_ref.shape, 0)
    hot_ref[...] = (at == place_ref[...]).astype(F32).astype(BF)


def hots(place, rows):
    tok = place.shape[1]
    return pl.pallas_call(
        hot_kernel,
        out_shape=jax.ShapeDtypeStruct((rows, tok), BF),
        compiler_params=pltpu.CompilerParams(vmem_limit_bytes=8 * 1024 * 1024),
        name="hots",
    )(place)


def mix_kernel(hot_ref, back_ref, *refs):
    out_ref, rows_ref = refs[-2:]
    flatten_rows(back_ref, rows_ref)
    out_ref[...] = lax.dot_general(
        hot_ref[...], rows_ref[...], (((0,), (0,)), ((), ())), preferred_element_type=F32
    ).astype(BF)


def mix(hot, returned, start, width, base):
    pairs, _, cols = returned.shape
    tok = hot.shape[1]
    block = 512
    first = start // block
    specs = [
        pl.BlockSpec(memory_space=pltpu.VMEM),
        pl.BlockSpec((pairs, 2, block), lambda j: (0, 0, j)),
    ]
    args, aliases = [hot, returned], {}
    if base is not None:
        aliases = {2: 0}
        args.append(base)
        specs.append(pl.BlockSpec(memory_space=pl.ANY))
    return pl.pallas_call(
        mix_kernel,
        grid=(cols // block,),
        in_specs=specs,
        out_specs=pl.BlockSpec((tok, block), lambda j: (0, j + first)),
        out_shape=jax.ShapeDtypeStruct((tok, width), BF),
        scratch_shapes=[pltpu.VMEM((2 * pairs, block), BF)],
        input_output_aliases=aliases,
        cost_estimate=pl.CostEstimate(flops=4 * tok * pairs * cols, bytes_accessed=4 * pairs * cols + 2 * tok * cols, transcendentals=0),
        compiler_params=pltpu.CompilerParams(vmem_limit_bytes=16 * 1024 * 1024),
        name="mix",
    )(*args)


def on_device(tokens, token_ids, table, w_in, w_out):
    experts = lax.axis_size("g") * lax.axis_size("y")
    tok_rows, width = tokens.shape
    slots = 2 * tok_rows // experts
    half = w_out.shape[1] // 2
    y = lax.axis_index("y")
    route = weight_route()
    swap = [(0, 1), (1, 0)]
    own_in = []
    for p in range(4):
        h, k = (y ^ p) >> 1, (y ^ p) & 1
        block = lax.dynamic_slice(w_in, (k, 0, h * half), (1, width, half))[0]
        own_in.append(lax.ppermute(block, ("c", "y"), route[p]))
    other_in = [lax.ppermute(o, "c", swap) for o in own_in]
    own_in = jnp.concatenate(own_in, axis=1)
    other_in = jnp.concatenate(other_in, axis=1)
    pieces = []
    for low, high in zip(CUTS[:-1], CUTS[1:]):
        own = []
        for p in range(4):
            h, k = (y ^ p) >> 1, (y ^ p) & 1
            block = lax.dynamic_slice(w_out, (k, h * half, low), (1, half, high - low))[0]
            own.append(lax.ppermute(block, ("c", "y"), route[p]))
        pieces.append(own + [lax.ppermute(o, "c", swap) for o in own])

    packed, place = pack(token_ids, table, tokens, experts, slots)
    arrived = lax.all_to_all(packed, ("g", "y"), split_axis=0, concat_axis=0, tiled=True)
    hidden = up(arrived, own_in, other_in)
    returned = []
    for j in range(len(CUTS) - 1):
        result = down(hidden, pieces[j])
        returned.append(lax.all_to_all(result, ("g", "y"), split_axis=0, concat_axis=0, tiled=True))
    hot = hots(place, experts * slots)
    mixed = None
    for j, low in enumerate(CUTS[:-1]):
        mixed = mix(hot, returned[j], low, width, mixed)
    return mixed


def solution(mesh):
    groups, pair = mesh.shape["expert"], mesh.shape["pair"]
    fine = Mesh(mesh.devices.reshape(groups // 2, 2, pair), ("g", "c", "y"))
    rows = ("g", "c", "y")
    in_specs = (
        P(rows, None),
        P(rows),
        P(),
        P(("g", "c"), None, "y"),
        P(("g", "c"), "y", None),
    )
    return jax.shard_map(on_device, mesh=fine, in_specs=in_specs, out_specs=P(rows, None), check_vma=False)
```

```python
import functools

import jax
import jax.numpy as jnp
from jax import lax
from jax.experimental import pallas as pl
from jax.experimental.pallas import tpu as pltpu
from jax.sharding import Mesh, PartitionSpec as P

BF = jnp.bfloat16
F32 = jnp.float32
CUTS = (0, 512, 2048)
UP_VMEM = 46 * 1024 * 1024


def weight_route():
    return [
        [(c * 4 + y, (y >> 1) * 4 + 2 * c + ((y ^ p) & 1)) for c in range(2) for y in range(4)]
        for p in range(2)
    ]


def pack_kernel(slots, ids_ref, table_ref, tok_ref, packed_ref, place_ref):
    rows, lanes = table_ref.shape
    tok = ids_ref.shape[1]
    pairs = packed_ref.shape[0]
    experts = 2 * pairs // slots
    ids = ids_ref[...]
    low = lax.rem(ids, lanes)
    high = lax.div(ids, lanes)
    low_hot = (lax.broadcasted_iota(jnp.int32, (lanes, tok), 0) == low).astype(F32).astype(BF)
    picked = jnp.dot(table_ref[...].astype(F32).astype(BF), low_hot, preferred_element_type=F32)
    high_hot = lax.broadcasted_iota(jnp.int32, (rows, tok), 0) == high
    chosen = jnp.sum(jnp.where(high_hot, picked, 0.0), axis=0, keepdims=True)
    hot = lax.broadcasted_iota(jnp.int32, (experts, tok), 0).astype(F32) == chosen
    before = (
        lax.broadcasted_iota(jnp.int32, (tok, tok), 0) < lax.broadcasted_iota(jnp.int32, (tok, tok), 1)
    ).astype(F32).astype(BF)
    earlier = jnp.dot(hot.astype(F32).astype(BF), before, preferred_element_type=F32)
    rank = jnp.sum(jnp.where(hot, earlier, 0.0), axis=0, keepdims=True)
    place = jnp.where(rank < slots, chosen * slots + rank, -1.0).astype(jnp.int32)
    place_ref[...] = place
    block = 128

    def step(i, _):
        at = lax.broadcasted_iota(jnp.int32, (block, tok), 0) + i * block
        onehot = (at == place).astype(F32).astype(BF)
        out = jnp.dot(onehot, tok_ref[...], preferred_element_type=F32).astype(BF)
        packed_ref[pl.ds(pl.multiple_of(i * (block // 2), block // 2), block // 2)] = out.reshape(block // 2, 2, out.shape[1])
        return 0

    lax.fori_loop(0, 2 * pairs // block, step, 0)


def pack(token_ids, table, tokens, experts, slots):
    tok, width = tokens.shape
    return pl.pallas_call(
        functools.partial(pack_kernel, slots),
        out_shape=(
            jax.ShapeDtypeStruct((experts * slots // 2, 2, width), BF),
            jax.ShapeDtypeStruct((1, tok), jnp.int32),
        ),
        cost_estimate=pl.CostEstimate(flops=2 * experts * slots * tok * width, bytes_accessed=6 * 1024 * 1024, transcendentals=0),
        compiler_params=pltpu.CompilerParams(vmem_limit_bytes=12 * 1024 * 1024),
        name="pack",
    )(token_ids.reshape(1, tok), table.reshape(-1, 128), tokens)


def flatten_rows(src_ref, dst_ref):
    pairs, _, width = src_ref.shape
    block = 16

    def step(i, _):
        part = src_ref[pl.ds(pl.multiple_of(i * block, block), block)]
        dst_ref[pl.ds(pl.multiple_of(i * 2 * block, 2 * block), 2 * block), :] = part.reshape(2 * block, width)
        return 0

    lax.fori_loop(0, pairs // block, step, 0)


def up_kernel(x_ref, own_ref, other_ref, hidden_ref, rows_ref):
    j = pl.program_id(0)

    @pl.when(j == 0)
    def _():
        flatten_rows(x_ref, rows_ref)

    def run(w_ref):
        out = jnp.dot(rows_ref[...], w_ref[...], preferred_element_type=F32)
        hidden_ref[...] = jnp.maximum(out, 0.0).astype(BF)

    half = pl.num_programs(0) // 2

    @pl.when(j < half)
    def _():
        run(own_ref)

    @pl.when(j >= half)
    def _():
        run(other_ref)


def up(arrived, own, other):
    pairs, _, width = arrived.shape
    units = own.shape[1]
    block = 256
    half = units // block
    return pl.pallas_call(
        up_kernel,
        grid=(2 * half,),
        in_specs=[
            pl.BlockSpec(memory_space=pltpu.VMEM),
            pl.BlockSpec((width, block), lambda j: (0, jnp.minimum(j, half - 1))),
            pl.BlockSpec((width, block), lambda j: (0, jnp.maximum(j - half, 0))),
        ],
        out_specs=pl.BlockSpec((2 * pairs, block), lambda j: (0, j)),
        out_shape=jax.ShapeDtypeStruct((2 * pairs, 2 * units), BF),
        scratch_shapes=[pltpu.VMEM((2 * pairs, width), BF)],
        cost_estimate=pl.CostEstimate(flops=8 * pairs * units * width, bytes_accessed=16 * 1024 * 1024, transcendentals=0),
        compiler_params=pltpu.CompilerParams(vmem_limit_bytes=UP_VMEM),
        name="up",
    )(arrived, own, other)


def down_kernel(n, hidden_ref, *refs):
    pieces, out_ref, w_ref = refs[:n], refs[-2], refs[-1]
    depth = pieces[0].shape[0]
    for p in range(n):
        w_ref[p * depth:(p + 1) * depth, :] = pieces[p][...]
    out = jnp.dot(hidden_ref[...], w_ref[...], preferred_element_type=F32).astype(BF)
    out_ref[...] = out.reshape(out_ref.shape)


def down(hidden, pieces):
    rows, units = hidden.shape
    depth, cols = pieces[0].shape
    n = len(pieces)
    block = 512
    return pl.pallas_call(
        functools.partial(down_kernel, n),
        grid=(cols // block,),
        in_specs=[pl.BlockSpec(memory_space=pltpu.VMEM)] + [pl.BlockSpec((depth, block), lambda j: (0, j)) for _ in range(n)],
        out_specs=pl.BlockSpec((rows // 2, 2, block), lambda j: (0, 0, j)),
        out_shape=jax.ShapeDtypeStruct((rows // 2, 2, cols), BF),
        scratch_shapes=[pltpu.VMEM((units, block), BF)],
        cost_estimate=pl.CostEstimate(
            flops=2 * rows * units * cols, bytes_accessed=2 * rows * (units + cols) + 2 * units * cols, transcendentals=0
        ),
        compiler_params=pltpu.CompilerParams(vmem_limit_bytes=20 * 1024 * 1024),
        name="down",
    )(hidden, *pieces)


def hot_kernel(place_ref, hot_ref):
    at = lax.broadcasted_iota(jnp.int32, hot_ref.shape, 0)
    hot_ref[...] = (at == place_ref[...]).astype(F32).astype(BF)


def hots(place, rows):
    tok = place.shape[1]
    return pl.pallas_call(
        hot_kernel,
        out_shape=jax.ShapeDtypeStruct((rows, tok), BF),
        compiler_params=pltpu.CompilerParams(vmem_limit_bytes=8 * 1024 * 1024),
        name="hots",
    )(place)


def mix_kernel(hot_ref, back_ref, *refs):
    out_ref, rows_ref = refs[-2:]
    flatten_rows(back_ref, rows_ref)
    out_ref[...] = lax.dot_general(
        hot_ref[...], rows_ref[...], (((0,), (0,)), ((), ())), preferred_element_type=F32
    ).astype(BF)


def mix(hot, returned, start, width, base):
    pairs, _, cols = returned.shape
    tok = hot.shape[1]
    block = 512
    first = start // block
    specs = [
        pl.BlockSpec(memory_space=pltpu.VMEM),
        pl.BlockSpec((pairs, 2, block), lambda j: (0, 0, j)),
    ]
    args, aliases = [hot, returned], {}
    if base is not None:
        aliases = {2: 0}
        args.append(base)
        specs.append(pl.BlockSpec(memory_space=pl.ANY))
    return pl.pallas_call(
        mix_kernel,
        grid=(cols // block,),
        in_specs=specs,
        out_specs=pl.BlockSpec((tok, block), lambda j: (0, j + first)),
        out_shape=jax.ShapeDtypeStruct((tok, width), BF),
        scratch_shapes=[pltpu.VMEM((2 * pairs, block), BF)],
        input_output_aliases=aliases,
        cost_estimate=pl.CostEstimate(flops=4 * tok * pairs * cols, bytes_accessed=4 * pairs * cols + 2 * tok * cols, transcendentals=0),
        compiler_params=pltpu.CompilerParams(vmem_limit_bytes=16 * 1024 * 1024),
        name="mix",
    )(*args)


def on_device(tokens, token_ids, table, w_in, w_out):
    experts = lax.axis_size("g") * lax.axis_size("y")
    tok_rows, width = tokens.shape
    slots = 2 * tok_rows // experts
    quarter = w_out.shape[1]
    y = lax.axis_index("y")
    route = weight_route()
    swap = [(0, 1), (1, 0)]
    own_in = []
    for p in range(2):
        block = lax.dynamic_slice(w_in, ((y ^ p) & 1, 0, 0), (1, width, quarter))[0]
        own_in.append(lax.ppermute(block, ("c", "y"), route[p]))
    other_in = [lax.ppermute(o, "c", swap) for o in own_in]
    own_in = jnp.concatenate(own_in, axis=1)
    other_in = jnp.concatenate(other_in, axis=1)
    pieces = []
    for low, high in zip(CUTS[:-1], CUTS[1:]):
        own = []
        for p in range(2):
            block = lax.dynamic_slice(w_out, ((y ^ p) & 1, 0, low), (1, quarter, high - low))[0]
            own.append(lax.ppermute(block, ("c", "y"), route[p]))
        pieces.append(own + [lax.ppermute(o, "c", swap) for o in own])

    packed, place = pack(token_ids, table, tokens, experts, slots)
    arrived = lax.all_to_all(packed, ("g", "y"), split_axis=0, concat_axis=0, tiled=True)
    hidden = up(arrived, own_in, other_in)
    returned = []
    for j in range(len(CUTS) - 1):
        result = down(hidden, pieces[j])
        returned.append(lax.all_to_all(result, ("g", "y"), split_axis=0, concat_axis=0, tiled=True))
    hot = hots(place, experts * slots)
    mixed = None
    for j, low in enumerate(CUTS[:-1]):
        mixed = mix(hot, returned[j], low, width, mixed)
    return mixed


def solution(mesh):
    groups, pair = mesh.shape["expert"], mesh.shape["pair"]
    fine = Mesh(mesh.devices.reshape(groups // 2, 2, pair), ("g", "c", "y"))
    rows = ("g", "c", "y")
    in_specs = (
        P(rows, None),
        P(rows),
        P(),
        P(("g", "c"), None, "y"),
        P(("g", "c"), "y", None),
    )
    return jax.shard_map(on_device, mesh=fine, in_specs=in_specs, out_specs=P(rows, None), check_vma=False)
```
